8 devices in a mesh: tp: 2 (over z, y), ep: 4 (over x, core).
Axes of the slice: x: 2, y: 2, z: 1, core: 2. Of those that a mesh axis runs over, the one named last changes fastest.
Arguments:
- x_tok: bfloat16 [32768, 512], P('ep')
- dy_tok: bfloat16 [32768, 512], P('ep')
- route_idx: int32 [32768, 2], P('ep')
- norm_scale: float32 [512], replicated
- w_router: float32 [512, 32], replicated
- w_gate: bfloat16 [32, 512, 2048], P('ep', None, 'tp')
- w_lin: bfloat16 [32, 512, 2048], P('ep', None, 'tp')
- w_out: bfloat16 [32, 2048, 512], P('ep', 'tp')
Outputs:
- output 1: bfloat16 [32768, 512], P('ep')
- output 2: float32 [2], replicated
- output 3: bfloat16 [32768, 512], P('ep')
- output 4: float32 [512], replicated
- output 5: float32 [512, 32], replicated
- output 6: float32 [32, 512, 2048], P('ep', None, 'tp')
- output 7: float32 [32, 512, 2048], P('ep', None, 'tp')
- output 8: float32 [32, 2048, 512], P('ep', 'tp')
All inputs are finite; a program needn't handle non-finite values.
Results may differ from the reference program's by a relative error of at most 0.0154704.
Values are sent between devices in bfloat16 or wider.
A program may use at most 1 GiB of HBM per device.

```python
import jax
import jax.numpy as jnp
from jax import lax

MODEL_DIM = 512
FF_DIM = 2048
EXPERTS = 32
TOK_DEV = 8192
GROUPS = 4
TOKENS = TOK_DEV * GROUPS
SLOT_CAP = (5 * TOK_DEV + 2 * EXPERTS - 1) // (2 * EXPERTS)
NORM_EPS = 1e-6
Z_COEF = 0.001
AUX_COEF = 0.01


def draw_routes(root_key, tok_count, expert_count):
    sub_keys = jax.random.split(root_key, 4)
    expert_order = jax.random.permutation(sub_keys[0], expert_count)
    pick_left = jax.random.randint(sub_keys[1], (tok_count,), 0, expert_count)
    pick_right = jax.random.randint(sub_keys[2], (tok_count,), 0, expert_count)
    first_ids = expert_order[jnp.minimum(pick_left, pick_right)]
    step_size = jax.random.randint(sub_keys[3], (tok_count,), 1, expert_count)
    second_ids = (first_ids + step_size) % expert_count
    return jnp.stack([first_ids, second_ids], axis=1).astype(jnp.int32)


def setup_inputs(seed: int = 0) -> dict:
    sub_keys = jax.random.split(jax.random.key(seed), 8)
    x_tok = jax.random.normal(sub_keys[0], (TOKENS, MODEL_DIM), jnp.float32).astype(jnp.bfloat16)
    dy_tok = (jax.random.normal(sub_keys[1], (TOKENS, MODEL_DIM), jnp.float32) * MODEL_DIM ** -0.5).astype(jnp.bfloat16)
    route_idx = draw_routes(sub_keys[2], TOKENS, EXPERTS)
    norm_scale = 1.0 + 0.3 * jax.random.normal(sub_keys[3], (MODEL_DIM,), jnp.float32)
    w_router = jax.random.normal(sub_keys[4], (MODEL_DIM, EXPERTS), jnp.float32) * (4.0 * MODEL_DIM ** -0.5)
    w_gate = (jax.random.normal(sub_keys[5], (EXPERTS, MODEL_DIM, FF_DIM), jnp.float32) * MODEL_DIM ** -0.5).astype(jnp.bfloat16)
    w_lin = (jax.random.normal(sub_keys[6], (EXPERTS, MODEL_DIM, FF_DIM), jnp.float32) * MODEL_DIM ** -0.5).astype(jnp.bfloat16)
    w_out = (jax.random.normal(sub_keys[7], (EXPERTS, FF_DIM, MODEL_DIM), jnp.float32) * (1.5 * FF_DIM ** -0.5)).astype(jnp.bfloat16)
    return {'x_tok': x_tok, 'dy_tok': dy_tok, 'route_idx': route_idx, 'norm_scale': norm_scale, 'w_router': w_router, 'w_gate': w_gate, 'w_lin': w_lin, 'w_out': w_out}


def gelu_fn(pre_act):
    return jax.nn.gelu(pre_act, approximate=True)


def route_slots(route_ids, experts, slot_cap, stride):
    expert_ids = jnp.arange(experts, dtype=jnp.int32)
    hit_first = (route_ids[:, 0:1] == expert_ids).astype(jnp.int32)
    hit_second = (route_ids[:, 1:2] == expert_ids).astype(jnp.int32)
    rank_first = jnp.cumsum(hit_first, axis=0) - hit_first
    rank_second = jnp.cumsum(hit_second, axis=0) - hit_second + jnp.sum(hit_first, axis=0)
    pos_first = jnp.sum(rank_first * hit_first, axis=1)
    pos_second = jnp.sum(rank_second * hit_second, axis=1)
    overflow = experts * stride
    slot_first = jnp.where(pos_first < slot_cap, route_ids[:, 0] * stride + pos_first, overflow)
    slot_second = jnp.where(pos_second < slot_cap, route_ids[:, 1] * stride + pos_second, overflow)
    return slot_first, slot_second


def slot_tables(slot_first, slot_second, gate_first, gate_second, slot_total):
    tok_count = slot_first.shape[0]
    tok_ids = jnp.arange(tok_count, dtype=jnp.int32)
    slot_tok = jnp.full((slot_total + 1,), tok_count, jnp.int32)
    slot_tok = slot_tok.at[slot_first].set(tok_ids).at[slot_second].set(tok_ids)
    slot_gate = jnp.zeros((slot_total + 1,), jnp.float32)
    slot_gate = slot_gate.at[slot_first].set(gate_first).at[slot_second].set(gate_second)
    return slot_tok[:slot_total], slot_gate[:slot_total]


def pick_rows(row_data, slot_index):
    return jnp.take(row_data, slot_index, axis=0, mode='fill', fill_value=0)


def reference(x_tok, dy_tok, route_idx, norm_scale, w_router, w_gate, w_lin, w_out):
    x_wide = x_tok.astype(jnp.float32)
    inv_rms = lax.rsqrt(jnp.mean(x_wide * x_wide, axis=-1, keepdims=True) + NORM_EPS)
    x_norm = x_wide * inv_rms
    u_tok = (x_norm * norm_scale).astype(jnp.bfloat16)
    u_wide = u_tok.astype(jnp.float32)
    logits = jnp.dot(u_wide, w_router, preferred_element_type=jnp.float32)
    log_norm = jax.nn.logsumexp(logits, axis=-1)
    router_prob = jnp.exp(logits - log_norm[:, None])
    expert_ids = jnp.arange(EXPERTS, dtype=jnp.int32)
    one_first = (route_idx[:, 0:1] == expert_ids).astype(jnp.float32)
    one_second = (route_idx[:, 1:2] == expert_ids).astype(jnp.float32)
    frac_first = jnp.sum(one_first, axis=0) / TOKENS
    mean_prob = jnp.sum(router_prob, axis=0) / TOKENS
    z_loss = Z_COEF * jnp.sum(log_norm * log_norm) / TOKENS
    aux_loss = AUX_COEF * EXPERTS * jnp.sum(frac_first * mean_prob)
    gate_first = jnp.sum(router_prob * one_first, axis=-1)
    gate_second = jnp.sum(router_prob * one_second, axis=-1)
    gate_total = gate_first + gate_second
    norm_first = gate_first / gate_total
    norm_second = gate_second / gate_total
    gate_wide = w_gate.astype(jnp.float32)
    lin_wide = w_lin.astype(jnp.float32)
    out_wide = w_out.astype(jnp.float32)

    def group_step(grad_acc, group_in):
        ids_grp, u_grp, dy_grp, first_grp, second_grp = group_in
        slot_first, slot_second = route_slots(ids_grp, EXPERTS, SLOT_CAP, SLOT_CAP)
        slot_tok, slot_gate = slot_tables(slot_first, slot_second, first_grp, second_grp, EXPERTS * SLOT_CAP)
        disp_rows = pick_rows(u_grp, slot_tok).reshape(EXPERTS, SLOT_CAP, MODEL_DIM).astype(jnp.float32)
        a_gate = jnp.einsum('ecd,edf->ecf', disp_rows, gate_wide)
        a_lin = jnp.einsum('ecd,edf->ecf', disp_rows, lin_wide)
        gelu_val, gelu_back = jax.vjp(gelu_fn, a_gate)
        hidden = (gelu_val * a_lin).astype(jnp.bfloat16).astype(jnp.float32)
        exp_out = jnp.einsum('ecf,efd->ecd', hidden, out_wide).astype(jnp.bfloat16)
        exp_out = exp_out.reshape(EXPERTS * SLOT_CAP, MODEL_DIM)
        out_first = pick_rows(exp_out, slot_first)
        out_second = pick_rows(exp_out, slot_second)
        do_slot = (pick_rows(dy_grp, slot_tok).astype(jnp.float32) * slot_gate[:, None]).astype(jnp.bfloat16)
        do_slot = do_slot.astype(jnp.float32).reshape(EXPERTS, SLOT_CAP, MODEL_DIM)
        d_hidden = jnp.einsum('ecd,efd->ecf', do_slot, out_wide)
        da_gate = gelu_back(d_hidden * a_lin)[0].astype(jnp.bfloat16).astype(jnp.float32)
        da_lin = (d_hidden * gelu_val).astype(jnp.bfloat16).astype(jnp.float32)
        du_slot = jnp.einsum('ecf,edf->ecd', da_gate, gate_wide) + jnp.einsum('ecf,edf->ecd', da_lin, lin_wide)
        du_slot = du_slot.astype(jnp.bfloat16).reshape(EXPERTS * SLOT_CAP, MODEL_DIM)
        du_exp = pick_rows(du_slot, slot_first).astype(jnp.float32) + pick_rows(du_slot, slot_second).astype(jnp.float32)
        acc_gate, acc_lin, acc_out = grad_acc
        acc_gate = acc_gate + jnp.einsum('ecd,ecf->edf', disp_rows, da_gate)
        acc_lin = acc_lin + jnp.einsum('ecd,ecf->edf', disp_rows, da_lin)
        acc_out = acc_out + jnp.einsum('ecf,ecd->efd', hidden, do_slot)
        return (acc_gate, acc_lin, acc_out), (out_first, out_second, du_exp)

    group_in = (route_idx.reshape(GROUPS, TOK_DEV, 2), u_tok.reshape(GROUPS, TOK_DEV, MODEL_DIM), dy_tok.reshape(GROUPS, TOK_DEV, MODEL_DIM), norm_first.reshape(GROUPS, TOK_DEV), norm_second.reshape(GROUPS, TOK_DEV))
    grad_init = (jnp.zeros((EXPERTS, MODEL_DIM, FF_DIM), jnp.float32), jnp.zeros((EXPERTS, MODEL_DIM, FF_DIM), jnp.float32), jnp.zeros((EXPERTS, FF_DIM, MODEL_DIM), jnp.float32))
    grad_sums, per_group = lax.scan(group_step, grad_init, group_in)
    d_gate, d_lin, d_out = grad_sums
    out_first = per_group[0].reshape(TOKENS, MODEL_DIM).astype(jnp.float32)
    out_second = per_group[1].reshape(TOKENS, MODEL_DIM).astype(jnp.float32)
    du_exp = per_group[2].reshape(TOKENS, MODEL_DIM)
    y_tok = (x_wide + norm_first[:, None] * out_first + norm_second[:, None] * out_second).astype(jnp.bfloat16)
    dy_wide = dy_tok.astype(jnp.float32)
    dn_first = jnp.sum(dy_wide * out_first, axis=-1)
    dn_second = jnp.sum(dy_wide * out_second, axis=-1)
    gate_mix = norm_first * dn_first + norm_second * dn_second
    aux_coef = AUX_COEF * EXPERTS * frac_first
    d_logits = router_prob * (aux_coef - jnp.sum(aux_coef * router_prob, axis=-1, keepdims=True))
    d_logits = d_logits + (2.0 * Z_COEF) * log_norm[:, None] * router_prob
    d_logits = d_logits + one_first * (norm_first * (dn_first - gate_mix))[:, None]
    d_logits = d_logits + one_second * (norm_second * (dn_second - gate_mix))[:, None]
    d_router = jnp.dot(u_wide.T, d_logits, preferred_element_type=jnp.float32)
    du_all = du_exp + jnp.dot(d_logits, w_router.T, preferred_element_type=jnp.float32)
    d_scale = jnp.sum(du_all * x_norm, axis=0)
    dx_norm = du_all * norm_scale
    dx_tok = (dy_wide + inv_rms * (dx_norm - x_norm * jnp.mean(dx_norm * x_norm, axis=-1, keepdims=True))).astype(jnp.bfloat16)
    losses = jnp.stack([z_loss, aux_loss])
    return (y_tok, losses, dx_tok, d_scale, d_router, d_gate, d_lin, d_out)
```

```python
import functools

import jax
import jax.numpy as jnp
from jax import lax
from jax.experimental import pallas as pl
from jax.experimental.pallas import tpu as pltpu
from jax.sharding import PartitionSpec as P


NORM_EPS = 1e-6
Z_COEF = 0.001
AUX_COEF = 0.01
GELU_C = 0.7978845608028654
GELU_A = 0.044715
LANES = 128
VMEM_LIMIT = 64 * 1024 * 1024 - 128 * 1024


def row_gather_kernel(split, blocks, tok_ref, side_ref, x_ref, dya_ref, dyb_ref, scale_ref, gate_ref,
                      u_ref, do_ref, table, rows_buf):
    step = pl.program_id(0)
    tok_block, width = x_ref.shape
    slices = width // LANES
    tile = 2 * slices
    slot_cap = u_ref.shape[1]

    @pl.when(step < blocks)
    def _():
        x_wide = x_ref[...].astype(jnp.float32)
        inv_rms = lax.rsqrt(jnp.mean(x_wide * x_wide, axis=-1, keepdims=True) + NORM_EPS)
        u_wide = (x_wide * inv_rms * scale_ref[...]).astype(jnp.bfloat16).astype(jnp.float32)
        if split:
            half = blocks // 2
            dy_val = jnp.where(step // half == side_ref[0], dya_ref[...], dyb_ref[...]).astype(jnp.float32)
        else:
            dy_val = dya_ref[...].astype(jnp.float32)
        base = pl.multiple_of(step * (tok_block * tile), tile)
        for k in range(slices):
            cols = slice(k * LANES, (k + 1) * LANES)
            table[pl.ds(base + k, tok_block, stride=tile), :] = u_wide[:, cols]
            table[pl.ds(base + slices + k, tok_block, stride=tile), :] = dy_val[:, cols]

    @pl.when(step == 0)
    def _():
        table[pl.ds(blocks * tok_block * tile, tile), :] = jnp.zeros((tile, LANES), jnp.float32)

    @pl.when(step >= blocks)
    def _():
        first = (step - blocks) * slot_cap
        unroll = 16 if slot_cap % 16 == 0 else 1

        def body(i, carry):
            for q in range(unroll):
                slot = i * unroll + q
                tok = tok_ref[first + slot]
                rows_buf[pl.ds(pl.multiple_of(slot * tile, tile), tile), :] = \
                    table[pl.ds(pl.multiple_of(tok * tile, tile), tile), :]
            return carry

        lax.fori_loop(0, slot_cap // unroll, body, 0)
        gate = gate_ref[0]
        for k in range(slices):
            cols = slice(k * LANES, (k + 1) * LANES)
            u_ref[0, :, cols] = rows_buf[pl.ds(k, slot_cap, stride=tile), :].astype(jnp.bfloat16)
            dy_rows = rows_buf[pl.ds(slices + k, slot_cap, stride=tile), :]
            do_ref[0, :, cols] = (dy_rows * gate).astype(jnp.bfloat16)


def gather_rows(slot_tok, side, x_grp, dy_parts, scale_row, gate_col):
    tok_count, width = x_grp.shape
    local_exp, slot_cap, _ = gate_col.shape
    tok_block = 512
    blocks = tok_count // tok_block
    half = blocks // 2
    tile = 2 * width // LANES
    split = len(dy_parts) == 2
    if split:
        dya, dyb = dy_parts
        map_a = lambda i, tok, sd: (jnp.clip(i - sd[0] * half, 0, half - 1), 0)
        map_b = lambda i, tok, sd: (jnp.clip(i - (1 - sd[0]) * half, 0, half - 1), 0)
    else:
        dya = dyb = dy_parts[0]
        map_a = lambda i, tok, sd: (jnp.minimum(i, blocks - 1), 0)
        map_b = lambda i, tok, sd: (0, 0)
    exp_map = lambda i, tok, sd: (jnp.maximum(i - blocks, 0), 0, 0)
    tok_spec = (tok_block, width)
    row_shape = jax.ShapeDtypeStruct((local_exp, slot_cap, width), jnp.bfloat16)
    return pl.pallas_call(
        functools.partial(row_gather_kernel, split, blocks),
        grid_spec=pltpu.PrefetchScalarGridSpec(
            num_scalar_prefetch=2,
            grid=(blocks + local_exp,),
            in_specs=[
                pl.BlockSpec(tok_spec, lambda i, tok, sd: (jnp.minimum(i, blocks - 1), 0)),
                pl.BlockSpec(tok_spec, map_a),
                pl.BlockSpec(tok_spec, map_b),
                pl.BlockSpec((1, width), lambda i, tok, sd: (0, 0)),
                pl.BlockSpec((1, slot_cap, 1), exp_map),
            ],
            out_specs=[pl.BlockSpec((1, slot_cap, width), exp_map)] * 2,
            scratch_shapes=[
                pltpu.VMEM(((tok_count + 1) * tile, LANES), jnp.float32),
                pltpu.VMEM((slot_cap * tile, LANES), jnp.float32),
            ],
        ),
        out_shape=[row_shape, row_shape],
        compiler_params=pltpu.CompilerParams(vmem_limit_bytes=VMEM_LIMIT, dimension_semantics=("arbitrary",)),
        cost_estimate=pl.CostEstimate(flops=30_000_000_000, bytes_accessed=40_000_000, transcendentals=0),
        name="gather_rows",
    )(slot_tok, side, x_grp, dya, dyb, scale_row, gate_col)


def dot_nt(lhs, rhs):
    return lax.dot_general(lhs, rhs, (((1,), (1,)), ((), ())), preferred_element_type=jnp.float32)


def dot_tn(lhs, rhs):
    return lax.dot_general(lhs, rhs, (((0,), (0,)), ((), ())), preferred_element_type=jnp.float32)


def dot_nn(lhs, rhs):
    return jnp.dot(lhs, rhs, preferred_element_type=jnp.float32)


def expert_kernel(side_ref, u_ref, do_ref, gate_ref, lin_ref, out_ref,
                  o_keep, o_send, du_keep, du_send, h_ref, da0_ref, da1_ref):
    width = u_ref.shape[2]
    ff = gate_ref.shape[2]
    chunk = 256
    u_rows = u_ref[0]
    do_rows = do_ref[0]
    o_acc = None
    du_acc = None
    for f in range(0, ff, chunk):
        cols = slice(f, f + chunk)
        a0 = dot_nn(u_rows, gate_ref[0, :, cols])
        a1 = dot_nn(u_rows, lin_ref[0, :, cols])
        dh = dot_nt(do_rows, out_ref[0, cols, :])
        sq = a0 * a0
        th = jnp.tanh(GELU_C * (a0 + GELU_A * (sq * a0)))
        cdf = 0.5 * (1.0 + th)
        gelu = a0 * cdf
        slope = cdf + (0.5 * GELU_C) * a0 * (1.0 - th * th) * (1.0 + (3.0 * GELU_A) * sq)
        h = (gelu * a1).astype(jnp.bfloat16)
        da0 = (dh * a1 * slope).astype(jnp.bfloat16)
        da1 = (dh * gelu).astype(jnp.bfloat16)
        h_ref[0, :, cols] = h
        da0_ref[0, :, cols] = da0
        da1_ref[0, :, cols] = da1
        o_part = dot_nn(h, out_ref[0, cols, :])
        du_part = dot_nt(da0, gate_ref[0, :, cols]) + dot_nt(da1, lin_ref[0, :, cols])
        o_acc = o_part if o_acc is None else o_acc + o_part
        du_acc = du_part if du_acc is None else du_acc + du_part
    half = width // 2
    low_side = side_ref[0] == 0
    for acc, keep, send in ((o_acc, o_keep, o_send), (du_acc, du_keep, du_send)):
        low = acc[:, :half].astype(jnp.bfloat16)
        high = acc[:, half:].astype(jnp.bfloat16)
        keep[0] = jnp.where(low_side, low, high)
        send[0] = jnp.where(low_side, high, low)


def run_experts(side, u_rows, do_rows, gate_loc, lin_loc, out_loc):
    local_exp, slot_cap, width = u_rows.shape
    ff = gate_loc.shape[2]
    exp_map = lambda e, sd: (e, 0, 0)
    row_block = pl.BlockSpec((1, slot_cap, width), exp_map)
    in_block = pl.BlockSpec((1, width, ff), exp_map)
    out_block = pl.BlockSpec((1, ff, width), exp_map)
    half_block = pl.BlockSpec((1, slot_cap, width // 2), exp_map)
    ff_block = pl.BlockSpec((1, slot_cap, ff), exp_map)
    half_shape = jax.ShapeDtypeStruct((local_exp, slot_cap, width // 2), jnp.bfloat16)
    ff_shape = jax.ShapeDtypeStruct((local_exp, slot_cap, ff), jnp.bfloat16)
    return pl.pallas_call(
        expert_kernel,
        grid_spec=pltpu.PrefetchScalarGridSpec(
            num_scalar_prefetch=1,
            grid=(local_exp,),
            in_specs=[row_block, row_block, in_block, in_block, out_block],
            out_specs=[half_block] * 4 + [ff_block] * 3,
        ),
        out_shape=[half_shape] * 4 + [ff_shape] * 3,
        compiler_params=pltpu.CompilerParams(vmem_limit_bytes=VMEM_LIMIT, dimension_semantics=("arbitrary",)),
        cost_estimate=pl.CostEstimate(flops=60_000_000_000, bytes_accessed=100_000_000, transcendentals=0),
        name="expert_pass",
    )(side, u_rows, do_rows, gate_loc, lin_loc, out_loc)


def weight_grad_kernel(groups, *refs):
    ins, (dg_ref, dl_ref, dw_ref) = refs[:5 * groups], refs[5 * groups:]
    d_gate = d_lin = d_out = None
    for g in range(groups):
        u_ref, do_ref, h_ref, da0_ref, da1_ref = ins[5 * g:5 * g + 5]
        pg = dot_tn(u_ref[0], da0_ref[0])
        pn = dot_tn(u_ref[0], da1_ref[0])
        po = dot_tn(h_ref[0], do_ref[0])
        d_gate = pg if d_gate is None else d_gate + pg
        d_lin = pn if d_lin is None else d_lin + pn
        d_out = po if d_out is None else d_out + po
    dg_ref[0] = d_gate
    dl_ref[0] = d_lin
    dw_ref[0] = d_out


def weight_grads(parts):
    local_exp, slot_cap, width = parts[0][0].shape
    ff = parts[0][2].shape[2]
    splits = 2
    ff_blk = ff // splits
    row_block = pl.BlockSpec((1, slot_cap, width), lambda e, f: (e, 0, 0))
    ff_block = pl.BlockSpec((1, slot_cap, ff_blk), lambda e, f: (e, 0, f))
    in_shape = jax.ShapeDtypeStruct((local_exp, width, ff), jnp.float32)
    out_shape = jax.ShapeDtypeStruct((local_exp, ff, width), jnp.float32)
    return pl.pallas_call(
        functools.partial(weight_grad_kernel, len(parts)),
        grid=(local_exp, splits),
        in_specs=[row_block, row_block, ff_block, ff_block, ff_block] * len(parts),
        out_specs=[pl.BlockSpec((1, width, ff_blk), lambda e, f: (e, 0, f)),
                   pl.BlockSpec((1, width, ff_blk), lambda e, f: (e, 0, f)),
                   pl.BlockSpec((1, ff_blk, width), lambda e, f: (e, f, 0))],
        out_shape=[in_shape, in_shape, out_shape],
        compiler_params=pltpu.CompilerParams(vmem_limit_bytes=VMEM_LIMIT,
                                             dimension_semantics=("arbitrary", "arbitrary")),
        cost_estimate=pl.CostEstimate(flops=80_000_000_000, bytes_accessed=250_000_000, transcendentals=0),
        name="weight_grads",
    )(*[a for part in parts for a in part])


def rows_to_cols(rows):
    return jnp.transpose(rows, (1, 0))


def lane_pack(cols, lanes=LANES):
    count = cols[0].shape[0]
    lane = lax.broadcasted_iota(jnp.int32, (count, lanes), 1)
    packed = jnp.zeros((count, lanes), jnp.float32)
    for i, col in enumerate(cols):
        packed = jnp.where(lane == i, col, packed)
    return jnp.transpose(packed, (1, 0))[:8]


def fill_table(step, steps_each, sources, table):
    blk, slot_cap, half = sources[0].shape
    slices = half // LANES
    for g, src in enumerate(sources):
        @pl.when(step // steps_each == g)
        def _():
            rows = blk * slot_cap
            vals = src[...].reshape(rows, half).astype(jnp.float32)
            base = pl.multiple_of(step * (rows * slices), 8)
            for k in range(slices):
                table[pl.ds(base + k, rows, stride=slices), :] = vals[:, k * LANES:(k + 1) * LANES]


def pick_table(table, buf, row_ref, first, count, slices):
    unroll = 16

    def body(i, carry):
        for q in range(unroll):
            tok = i * unroll + q
            buf[pl.ds(pl.multiple_of(tok * slices, slices), slices), :] = \
                table[pl.ds(pl.multiple_of(row_ref[first + tok] * slices, slices), slices), :]
        return carry

    lax.fori_loop(0, count // unroll, body, 0)


def buf_slice(buf, k, count, slices):
    return buf[pl.ds(k, count, stride=slices), :]


def combine_o_kernel(table_steps, groups, row1_ref, row2_ref, side_ref, *refs):
    sources, (x_ref, dy_ref, feat_ref, y_ref, part_ref, table, buf1, buf2) = refs[:groups], refs[groups:]
    step = pl.program_id(0)
    count, half = x_ref.shape
    slices = half // LANES

    @pl.when(step == 0)
    def _():
        zero_at = table.shape[0] - 8
        table[pl.ds(zero_at, 8), :] = jnp.zeros((8, LANES), jnp.float32)

    @pl.when(step < table_steps)
    def _():
        fill_table(step, table_steps // groups, sources, table)

    @pl.when(step >= table_steps)
    def _():
        first = (step - table_steps) * count
        pick_table(table, buf1, row1_ref, first, count, slices)
        pick_table(table, buf2, row2_ref, first, count, slices)
        feat = rows_to_cols(feat_ref[...])
        n1, n2 = feat[:, 0:1], feat[:, 1:2]
        dn1 = dn2 = 0.0
        for k in range(slices):
            cols = slice(k * LANES, (k + 1) * LANES)
            o1 = buf_slice(buf1, k, count, slices)
            o2 = buf_slice(buf2, k, count, slices)
            dy = dy_ref[:, cols].astype(jnp.float32)
            y_ref[:, cols] = (x_ref[:, cols].astype(jnp.float32) + n1 * o1 + n2 * o2).astype(jnp.bfloat16)
            dn1 = dn1 + dy * o1
            dn2 = dn2 + dy * o2
        part_ref[...] = lane_pack([jnp.sum(dn1, axis=-1, keepdims=True), jnp.sum(dn2, axis=-1, keepdims=True)])


def combine_du_kernel(table_steps, groups, row1_ref, row2_ref, side_ref, *refs):
    sources = refs[:groups]
    (x_ref, feat_ref, dl_ref, wr_ref, scale_ref, du_ref, part_ref, dr_ref, ds_ref, table, buf1, buf2) = refs[groups:]
    step = pl.program_id(0)
    count, half = x_ref.shape
    slices = half // LANES

    @pl.when(step == 0)
    def _():
        zero_at = table.shape[0] - 8
        table[pl.ds(zero_at, 8), :] = jnp.zeros((8, LANES), jnp.float32)
        dr_ref[...] = jnp.zeros_like(dr_ref)
        ds_ref[...] = jnp.zeros_like(ds_ref)

    @pl.when(step < table_steps)
    def _():
        fill_table(step, table_steps // groups, sources, table)

    @pl.when(step >= table_steps)
    def _():
        first = (step - table_steps) * count
        pick_table(table, buf1, row1_ref, first, count, slices)
        pick_table(table, buf2, row2_ref, first, count, slices)
        inv_rms = rows_to_cols(feat_ref[...])[:, 2:3]
        d_logits = dl_ref[...]
        routed = lax.dot_general(d_logits, wr_ref[...], (((0,), (0,)), ((), ())), preferred_element_type=jnp.float32)
        dot = 0.0
        norm_in = []
        for k in range(slices):
            cols = slice(k * LANES, (k + 1) * LANES)
            du_exp = buf_slice(buf1, k, count, slices) + buf_slice(buf2, k, count, slices)
            xn = x_ref[:, cols].astype(jnp.float32) * inv_rms
            scaled = xn * scale_ref[:, cols]
            du_all = du_exp + routed[:, cols]
            du_ref[:, cols] = du_all
            dot = dot + du_all * scaled
            ds_ref[:, cols] += jnp.sum(du_all * xn, axis=0, keepdims=True)
            norm_in.append(scaled.astype(jnp.bfloat16).astype(jnp.float32))
        part_ref[...] = lane_pack([jnp.sum(dot, axis=-1, keepdims=True)])
        dr_ref[...] += jnp.dot(d_logits, jnp.concatenate(norm_in, axis=1), preferred_element_type=jnp.float32)


def finish_dx_kernel(side_ref, du_ref, x_ref, dy_ref, feat_ref, part_a_ref, part_b_ref, scale_ref, dx_ref):
    width = 2 * x_ref.shape[1]
    inv_rms = rows_to_cols(feat_ref[...])[:, 2:3]
    mean = rows_to_cols(part_a_ref[...] + part_b_ref[...])[:, 0:1] * (1.0 / width)
    xn = x_ref[...].astype(jnp.float32) * inv_rms
    grad = dy_ref[...].astype(jnp.float32) + inv_rms * (du_ref[...] * scale_ref[...] - xn * mean)
    dx_ref[...] = grad.astype(jnp.bfloat16)


TOK_BLOCK = 512


def half_specs(offset):
    at = lambda i: jnp.maximum(i - offset, 0)
    tok = lambda i, r1, r2, sd: (at(i), 0)
    half_tok = lambda i, r1, r2, sd: (at(i), sd[0])
    row = lambda i, r1, r2, sd: (0, at(i))
    return tok, half_tok, row


def combine_call(kernel, rows, side, sources, extra, extra_specs, outs, out_specs, tok_count):
    local_exp, slot_cap, half = sources[0].shape
    groups = len(sources)
    blk = 2
    each = local_exp // blk
    table_steps = groups * each
    slices = half // LANES
    src_specs = [pl.BlockSpec((blk, slot_cap, half), (lambda g: lambda i, r1, r2, sd: (jnp.clip(i - g * each, 0, each - 1), 0, 0))(g))
                 for g in range(groups)]
    return pl.pallas_call(
        functools.partial(kernel, table_steps, groups),
        grid_spec=pltpu.PrefetchScalarGridSpec(
            num_scalar_prefetch=3,
            grid=(table_steps + tok_count // TOK_BLOCK,),
            in_specs=src_specs + extra_specs(table_steps),
            out_specs=out_specs(table_steps),
            scratch_shapes=[
                pltpu.VMEM((groups * local_exp * slot_cap * slices + 8, LANES), jnp.float32),
                pltpu.VMEM((TOK_BLOCK * slices, LANES), jnp.float32),
                pltpu.VMEM((TOK_BLOCK * slices, LANES), jnp.float32),
            ],
        ),
        out_shape=outs,
        compiler_params=pltpu.CompilerParams(vmem_limit_bytes=VMEM_LIMIT, dimension_semantics=("arbitrary",)),
        cost_estimate=pl.CostEstimate(flops=50_000_000_000, bytes_accessed=40_000_000, transcendentals=0),
    )(rows[0], rows[1], side, *sources, *extra)


def combine_o(rows, side, sources, x_loc, dy_loc, feat):
    tok_count, width = x_loc.shape
    half = width // 2

    def ins(offset):
        _, half_tok, row = half_specs(offset)
        return [pl.BlockSpec((TOK_BLOCK, half), half_tok)] * 2 + [pl.BlockSpec((8, TOK_BLOCK), row)]

    def out_specs(offset):
        tok, _, row = half_specs(offset)
        return [pl.BlockSpec((TOK_BLOCK, half), tok), pl.BlockSpec((8, TOK_BLOCK), row)]

    outs = [jax.ShapeDtypeStruct((tok_count, half), jnp.bfloat16), jax.ShapeDtypeStruct((8, tok_count), jnp.float32)]
    return combine_call(combine_o_kernel, rows, side, sources, (x_loc, dy_loc, feat), ins, outs, out_specs, tok_count)


def combine_du(rows, side, sources, x_loc, feat, d_logits_t, router_half_t, scale_half):
    tok_count, width = x_loc.shape
    half = width // 2
    experts = d_logits_t.shape[0]
    whole = lambda i, r1, r2, sd: (0, 0)

    def ins(offset):
        _, half_tok, row = half_specs(offset)
        return [pl.BlockSpec((TOK_BLOCK, half), half_tok), pl.BlockSpec((8, TOK_BLOCK), row),
                pl.BlockSpec((experts, TOK_BLOCK), row), pl.BlockSpec((experts, half), whole),
                pl.BlockSpec((1, half), whole)]

    def out_specs(offset):
        tok, _, row = half_specs(offset)
        return [pl.BlockSpec((TOK_BLOCK, half), tok), pl.BlockSpec((8, TOK_BLOCK), row),
                pl.BlockSpec((experts, half), whole), pl.BlockSpec((1, half), whole)]

    outs = [jax.ShapeDtypeStruct((tok_count, half), jnp.float32), jax.ShapeDtypeStruct((8, tok_count), jnp.float32),
            jax.ShapeDtypeStruct((experts, half), jnp.float32), jax.ShapeDtypeStruct((1, half), jnp.float32)]
    return combine_call(combine_du_kernel, rows, side, sources,
                        (x_loc, feat, d_logits_t, router_half_t, scale_half), ins, outs, out_specs, tok_count)


def finish_dx(side, du_all, x_loc, dy_loc, feat, part_a, part_b, scale_half):
    tok_count, half = du_all.shape
    tok = lambda i, sd: (i, 0)
    half_tok = lambda i, sd: (i, sd[0])
    row = lambda i, sd: (0, i)
    return pl.pallas_call(
        finish_dx_kernel,
        grid_spec=pltpu.PrefetchScalarGridSpec(
            num_scalar_prefetch=1,
            grid=(tok_count // TOK_BLOCK,),
            in_specs=[pl.BlockSpec((TOK_BLOCK, half), tok), pl.BlockSpec((TOK_BLOCK, half), half_tok),
                      pl.BlockSpec((TOK_BLOCK, half), half_tok)] + [pl.BlockSpec((8, TOK_BLOCK), row)] * 3 +
                     [pl.BlockSpec((1, half), lambda i, sd: (0, 0))],
            out_specs=pl.BlockSpec((TOK_BLOCK, half), tok),
        ),
        out_shape=jax.ShapeDtypeStruct((tok_count, half), jnp.bfloat16),
        compiler_params=pltpu.CompilerParams(vmem_limit_bytes=VMEM_LIMIT, dimension_semantics=("arbitrary",)),
        cost_estimate=pl.CostEstimate(flops=10_000_000_000, bytes_accessed=20_000_000, transcendentals=0),
        name="finish_dx",
    )(side, du_all, x_loc, dy_loc, feat, part_a, part_b, scale_half)


def slot_positions(hit_first, hit_second):
    rank_first = jnp.cumsum(hit_first, axis=0) - hit_first
    rank_second = jnp.cumsum(hit_second, axis=0) - hit_second + jnp.sum(hit_first, axis=0)
    return jnp.sum(rank_first * hit_first, axis=1), jnp.sum(rank_second * hit_second, axis=1)


def round_bf16(val):
    return lax.reduce_precision(val, 8, 7)


def solution(mesh):
    ep_size = mesh.shape['ep']
    tp_size = mesh.shape['tp']

    def swap_ep(val, bit):
        return lax.ppermute(val, 'ep', [(i, i ^ bit) for i in range(ep_size)])

    def swap_tp(val):
        return lax.ppermute(val, 'tp', [(i, i ^ 1) for i in range(tp_size)])

    def device_body(x_loc, dy_loc, idx_loc, norm_scale, w_router, gate_loc, lin_loc, out_loc):
        tok_count, width = x_loc.shape
        experts = w_router.shape[1]
        local_exp = gate_loc.shape[0]
        tokens = tok_count * ep_size
        slot_cap = (5 * tok_count + 2 * experts - 1) // (2 * experts)
        half = width // 2
        me = lax.axis_index('ep')
        side = lax.axis_index('tp')
        side_arr = side.astype(jnp.int32).reshape(1)

        dy_half = lax.dynamic_slice_in_dim(dy_loc, side * (tok_count // 2), tok_count // 2, axis=0)
        dy2_a = swap_ep(dy_half, 2)
        x2 = swap_ep(x_loc, 2)
        dy2_b = swap_tp(dy2_a)
        x1 = swap_ep(x_loc, 1)
        dy1 = swap_ep(dy_loc, 1)
        x3 = swap_ep(x2, 1)
        dy3_a = swap_ep(dy2_a, 1)
        dy3_b = swap_ep(dy2_b, 1)
        x_grp = (x_loc, x1, x2, x3)
        dy_grp = ((dy_loc,), (dy1,), (dy2_a, dy2_b), (dy3_a, dy3_b))

        x_wide = x_loc.astype(jnp.float32)
        inv_rms = lax.rsqrt(jnp.mean(x_wide * x_wide, axis=-1, keepdims=True) + NORM_EPS)
        u_tok = (x_wide * inv_rms * norm_scale).astype(jnp.bfloat16)
        u_wide = u_tok.astype(jnp.float32)
        logits = jnp.dot(u_wide, w_router, preferred_element_type=jnp.float32)
        log_norm = jax.nn.logsumexp(logits, axis=-1)
        router_prob = jnp.exp(logits - log_norm[:, None])
        expert_ids = jnp.arange(experts, dtype=jnp.int32)
        hit_first = idx_loc[:, 0:1] == expert_ids
        hit_second = idx_loc[:, 1:2] == expert_ids
        one_first = hit_first.astype(jnp.float32)
        one_second = hit_second.astype(jnp.float32)
        gate_first = jnp.sum(router_prob * one_first, axis=-1)
        gate_second = jnp.sum(router_prob * one_second, axis=-1)
        gate_total = gate_first + gate_second
        norm_first = gate_first / gate_total
        norm_second = gate_second / gate_total

        pos_first, pos_second = slot_positions(hit_first.astype(jnp.int32), hit_second.astype(jnp.int32))
        tok_ids = jnp.arange(tok_count, dtype=jnp.int32)
        tok_hi = (tok_ids // 64).astype(jnp.float32)
        tok_lo = (tok_ids % 64).astype(jnp.float32)
        slot_ids = jnp.arange(slot_cap, dtype=jnp.int32)
        table = 0.0
        for one, pos, norm in ((one_first, pos_first, norm_first), (one_second, pos_second, norm_second)):
            g_hi = round_bf16(norm)
            g_mid = round_bf16(norm - g_hi)
            g_lo = round_bf16(norm - g_hi - g_mid)
            feats = [jnp.ones_like(norm), tok_hi, tok_lo, g_hi, g_mid, g_lo]
            left = jnp.concatenate([one * f[:, None] for f in feats], axis=1).astype(jnp.bfloat16)
            right = (pos[:, None] == slot_ids).astype(jnp.bfloat16)
            table = table + lax.dot_general(left, right, (((0,), (0,)), ((), ())), preferred_element_type=jnp.float32)
        table = table.reshape(6, experts, slot_cap)
        slot_tok = jnp.where(table[0] > 0.5, table[1] * 64.0 + table[2], float(tok_count))
        slot_gate = table[3] + table[4] + table[5]
        slot_pack = jnp.stack([slot_tok, slot_gate]).reshape(2, ep_size, local_exp, slot_cap)

        scale_row = norm_scale.reshape(1, width)
        saved = {}
        back_o = [None] * ep_size
        back_du = [None] * ep_size
        sent = {}
        for bit in range(ep_size):
            pack = lax.dynamic_index_in_dim(slot_pack, me ^ bit, axis=1, keepdims=False)
            if bit:
                pack = swap_ep(pack, bit)
            tok_grp = pack[0].astype(jnp.int32).reshape(local_exp * slot_cap)
            gate_grp = pack[1].reshape(local_exp, slot_cap, 1)
            u_rows, do_rows = gather_rows(tok_grp, side_arr, x_grp[bit], dy_grp[bit], scale_row, gate_grp)
            o_keep, o_send, du_keep, du_send, h, da0, da1 = run_experts(
                side_arr, u_rows, do_rows, gate_loc, lin_loc, out_loc)
            saved[bit] = (u_rows, do_rows, h, da0, da1)
            sent[bit] = (o_keep, o_send, du_keep, du_send)
        for bit in range(ep_size):
            o_keep, o_send, du_keep, du_send = sent[bit]
            o_got = swap_tp(o_send)
            du_got = swap_tp(du_send)
            o_sum = (o_keep.astype(jnp.float32) + o_got.astype(jnp.float32)).astype(jnp.bfloat16)
            du_sum = (du_keep.astype(jnp.float32) + du_got.astype(jnp.float32)).astype(jnp.bfloat16)
            if bit:
                o_sum = swap_ep(o_sum, bit)
                du_sum = swap_ep(du_sum, bit)
            back_o[bit] = o_sum
            back_du[bit] = du_sum
        d_gate, d_lin, d_out = weight_grads([saved[b] for b in range(ep_size)])

        per_dev = local_exp * slot_cap

        def slot_row(exp_idx, pos):
            row = ((exp_idx // local_exp) ^ me) * per_dev + (exp_idx % local_exp) * slot_cap + pos
            return jnp.where(pos < slot_cap, row, ep_size * per_dev)

        rows = (slot_row(idx_loc[:, 0], pos_first), slot_row(idx_loc[:, 1], pos_second))
        half_of = lambda val, axis: lax.dynamic_slice_in_dim(val, side * half, half, axis=axis)
        scale_half = half_of(norm_scale, 0)[None, :]
        zero_row = jnp.zeros_like(norm_first)
        feat = jnp.stack([norm_first, norm_second, inv_rms[:, 0]] + [zero_row] * 5)
        y_half, part_o = combine_o(rows, side_arr, back_o, x_loc, dy_loc, feat)
        y_other = swap_tp(y_half)
        part_o = part_o + swap_tp(part_o)
        dn_first, dn_second = part_o[0], part_o[1]

        stats = jnp.concatenate([jnp.sum(one_first, axis=0), jnp.sum(router_prob, axis=0),
                                 jnp.sum(log_norm * log_norm).reshape(1)])
        stats = lax.psum(stats, 'ep')
        first_count, prob_sum, norm_sq = stats[:experts], stats[experts:2 * experts], stats[2 * experts]
        frac_first = first_count / tokens
        z_loss = Z_COEF * norm_sq / tokens
        aux_loss = AUX_COEF * experts * jnp.sum(frac_first * prob_sum) / tokens
        gate_mix = norm_first * dn_first + norm_second * dn_second
        aux_coef = AUX_COEF * experts * frac_first
        d_logits = router_prob * (aux_coef - jnp.sum(aux_coef * router_prob, axis=-1, keepdims=True))
        d_logits = d_logits + (2.0 * Z_COEF) * log_norm[:, None] * router_prob
        d_logits = d_logits + one_first * (norm_first * (dn_first - gate_mix))[:, None]
        d_logits = d_logits + one_second * (norm_second * (dn_second - gate_mix))[:, None]

        du_all, part_du, d_router_half, d_scale_half = combine_du(
            rows, side_arr, back_du, x_loc, feat, d_logits.T, half_of(w_router, 0).T, scale_half)
        part_other = swap_tp(part_du)
        dx_half = finish_dx(side_arr, du_all, x_loc, dy_loc, feat, part_du, part_other, scale_half)
        sums = jnp.concatenate([d_router_half, d_scale_half])
        dx_half, sums = lax.optimization_barrier((dx_half, sums))
        dx_other = swap_tp(dx_half)
        sums = lax.dynamic_update_slice_in_dim(jnp.zeros((experts + 1, width), jnp.float32), sums, side * half, axis=1)
        sums = lax.psum(sums, ('ep', 'tp'))
        d_router = sums[:experts].T
        d_scale = sums[experts]

        def join(mine, other):
            return jnp.where(side == 0, jnp.concatenate([mine, other], axis=1), jnp.concatenate([other, mine], axis=1))

        y_loc = join(y_half, y_other)
        dx_loc = join(dx_half, dx_other)
        losses = jnp.stack([z_loss, aux_loss])
        return (y_loc, losses, dx_loc, d_scale, d_router, d_gate, d_lin, d_out)

    tok_spec = P('ep', None)
    in_spec = P('ep', None, 'tp')
    out_spec = P('ep', 'tp', None)
    return jax.shard_map(device_body, mesh=mesh, in_specs=(tok_spec, tok_spec, tok_spec, P(), P(), in_spec, in_spec, out_spec), out_specs=(tok_spec, P(), tok_spec, P(), P(), in_spec, in_spec, out_spec), check_vma=False)
```

```python
import functools

import jax
import jax.numpy as jnp
from jax import lax
from jax.experimental import pallas as pl
from jax.experimental.pallas import tpu as pltpu
from jax.sharding import PartitionSpec as P


NORM_EPS = 1e-6
Z_COEF = 0.001
AUX_COEF = 0.01
GELU_C = 0.7978845608028654
GELU_A = 0.044715
LANES = 128
VMEM_LIMIT = 64 * 1024 * 1024 - 128 * 1024


def part_slot(p, part_count, side):
    if part_count == 1:
        return 0
    per_half = part_count // 2
    own = p < per_half
    return (side if own else 1 - side) * per_half + p % per_half


def row_gather_kernel(part_count, blocks, tok_ref, side_ref, x_ref, *refs):
    dy_refs, (scale_ref, gate_ref, u_ref, do_ref, table, rows_buf) = refs[:part_count], refs[part_count:]
    step = pl.program_id(0)
    tok_block, width = x_ref.shape
    slices = width // LANES
    tile = 2 * slices
    slot_cap = u_ref.shape[1]

    @pl.when(step < blocks)
    def _():
        x_wide = x_ref[...].astype(jnp.float32)
        inv_rms = lax.rsqrt(jnp.mean(x_wide * x_wide, axis=-1, keepdims=True) + NORM_EPS)
        u_wide = (x_wide * inv_rms * scale_ref[...]).astype(jnp.bfloat16).astype(jnp.float32)
        dy_val = dy_refs[0][...]
        for p in range(1, part_count):
            dy_val = jnp.where(step // (blocks // part_count) == part_slot(p, part_count, side_ref[0]), dy_refs[p][...], dy_val)
        dy_val = dy_val.astype(jnp.float32)
        base = pl.multiple_of(step * (tok_block * tile), tile)
        for k in range(slices):
            cols = slice(k * LANES, (k + 1) * LANES)
            table[pl.ds(base + k, tok_block, stride=tile), :] = u_wide[:, cols]
            table[pl.ds(base + slices + k, tok_block, stride=tile), :] = dy_val[:, cols]

    @pl.when(step == 0)
    def _():
        table[pl.ds(blocks * tok_block * tile, tile), :] = jnp.zeros((tile, LANES), jnp.float32)

    @pl.when(step >= blocks)
    def _():
        first = (step - blocks) * slot_cap
        unroll = 16 if slot_cap % 16 == 0 else 1

        def body(i, carry):
            for q in range(unroll):
                slot = i * unroll + q
                tok = tok_ref[first + slot]
                rows_buf[pl.ds(pl.multiple_of(slot * tile, tile), tile), :] = \
                    table[pl.ds(pl.multiple_of(tok * tile, tile), tile), :]
            return carry

        lax.fori_loop(0, slot_cap // unroll, body, 0)
        gate = gate_ref[0]
        for k in range(slices):
            cols = slice(k * LANES, (k + 1) * LANES)
            u_ref[0, :, cols] = rows_buf[pl.ds(k, slot_cap, stride=tile), :].astype(jnp.bfloat16)
            dy_rows = rows_buf[pl.ds(slices + k, slot_cap, stride=tile), :]
            do_ref[0, :, cols] = (dy_rows * gate).astype(jnp.bfloat16)


def gather_rows(slot_tok, side, x_grp, dy_parts, scale_row, gate_col):
    tok_count, width = x_grp.shape
    local_exp, slot_cap, _ = gate_col.shape
    tok_block = 512
    blocks = tok_count // tok_block
    tile = 2 * width // LANES
    part_count = len(dy_parts)
    each = blocks // part_count
    part_maps = [(lambda p: lambda i, tok, sd: (jnp.clip(i - part_slot(p, part_count, sd[0]) * each, 0, each - 1), 0))(p)
                 for p in range(part_count)]
    exp_map = lambda i, tok, sd: (jnp.maximum(i - blocks, 0), 0, 0)
    tok_spec = (tok_block, width)
    row_shape = jax.ShapeDtypeStruct((local_exp, slot_cap, width), jnp.bfloat16)
    return pl.pallas_call(
        functools.partial(row_gather_kernel, part_count, blocks),
        grid_spec=pltpu.PrefetchScalarGridSpec(
            num_scalar_prefetch=2,
            grid=(blocks + local_exp,),
            in_specs=[
                pl.BlockSpec(tok_spec, lambda i, tok, sd: (jnp.minimum(i, blocks - 1), 0)),
                *[pl.BlockSpec(tok_spec, m) for m in part_maps],
                pl.BlockSpec((1, width), lambda i, tok, sd: (0, 0)),
                pl.BlockSpec((1, slot_cap, 1), exp_map),
            ],
            out_specs=[pl.BlockSpec((1, slot_cap, width), exp_map)] * 2,
            scratch_shapes=[
                pltpu.VMEM(((tok_count + 1) * tile, LANES), jnp.float32),
                pltpu.VMEM((slot_cap * tile, LANES), jnp.float32),
            ],
        ),
        out_shape=[row_shape, row_shape],
        compiler_params=pltpu.CompilerParams(vmem_limit_bytes=VMEM_LIMIT, dimension_semantics=("arbitrary",)),
        cost_estimate=pl.CostEstimate(flops=30_000_000_000, bytes_accessed=40_000_000, transcendentals=0),
        name="gather_rows",
    )(slot_tok, side, x_grp, *dy_parts, scale_row, gate_col)


def dot_nt(lhs, rhs):
    return lax.dot_general(lhs, rhs, (((1,), (1,)), ((), ())), preferred_element_type=jnp.float32)


def dot_tn(lhs, rhs):
    return lax.dot_general(lhs, rhs, (((0,), (0,)), ((), ())), preferred_element_type=jnp.float32)


def dot_nn(lhs, rhs):
    return jnp.dot(lhs, rhs, preferred_element_type=jnp.float32)


def expert_kernel(side_ref, u_ref, do_ref, gate_ref, lin_ref, out_ref,
                  o_keep, o_send, du_keep, du_send, h_ref, da0_ref, da1_ref):
    width = u_ref.shape[2]
    ff = gate_ref.shape[2]
    chunk = 256
    u_rows = u_ref[0]
    do_rows = do_ref[0]
    o_acc = None
    du_acc = None
    for f in range(0, ff, chunk):
        cols = slice(f, f + chunk)
        a0 = dot_nn(u_rows, gate_ref[0, :, cols])
        a1 = dot_nn(u_rows, lin_ref[0, :, cols])
        dh = dot_nt(do_rows, out_ref[0, cols, :])
        sq = a0 * a0
        th = jnp.tanh(GELU_C * (a0 + GELU_A * (sq * a0)))
        cdf = 0.5 * (1.0 + th)
        gelu = a0 * cdf
        slope = cdf + (0.5 * GELU_C) * a0 * (1.0 - th * th) * (1.0 + (3.0 * GELU_A) * sq)
        h = (gelu * a1).astype(jnp.bfloat16)
        da0 = (dh * a1 * slope).astype(jnp.bfloat16)
        da1 = (dh * gelu).astype(jnp.bfloat16)
        h_ref[0, :, cols] = h
        da0_ref[0, :, cols] = da0
        da1_ref[0, :, cols] = da1
        o_part = dot_nn(h, out_ref[0, cols, :])
        du_part = dot_nt(da0, gate_ref[0, :, cols]) + dot_nt(da1, lin_ref[0, :, cols])
        o_acc = o_part if o_acc is None else o_acc + o_part
        du_acc = du_part if du_acc is None else du_acc + du_part
    half = width // 2
    low_side = side_ref[0] == 0
    for acc, keep, send in ((o_acc, o_keep, o_send), (du_acc, du_keep, du_send)):
        low = acc[:, :half].astype(jnp.bfloat16)
        high = acc[:, half:].astype(jnp.bfloat16)
        keep[0] = jnp.where(low_side, low, high)
        send[0] = jnp.where(low_side, high, low)


def run_experts(side, u_rows, do_rows, gate_loc, lin_loc, out_loc):
    local_exp, slot_cap, width = u_rows.shape
    ff = gate_loc.shape[2]
    exp_map = lambda e, sd: (e, 0, 0)
    row_block = pl.BlockSpec((1, slot_cap, width), exp_map)
    in_block = pl.BlockSpec((1, width, ff), exp_map)
    out_block = pl.BlockSpec((1, ff, width), exp_map)
    half_block = pl.BlockSpec((1, slot_cap, width // 2), exp_map)
    ff_block = pl.BlockSpec((1, slot_cap, ff), exp_map)
    half_shape = jax.ShapeDtypeStruct((local_exp, slot_cap, width // 2), jnp.bfloat16)
    ff_shape = jax.ShapeDtypeStruct((local_exp, slot_cap, ff), jnp.bfloat16)
    return pl.pallas_call(
        expert_kernel,
        grid_spec=pltpu.PrefetchScalarGridSpec(
            num_scalar_prefetch=1,
            grid=(local_exp,),
            in_specs=[row_block, row_block, in_block, in_block, out_block],
            out_specs=[half_block] * 4 + [ff_block] * 3,
        ),
        out_shape=[half_shape] * 4 + [ff_shape] * 3,
        compiler_params=pltpu.CompilerParams(vmem_limit_bytes=VMEM_LIMIT, dimension_semantics=("arbitrary",)),
        cost_estimate=pl.CostEstimate(flops=60_000_000_000, bytes_accessed=100_000_000, transcendentals=0),
        name="expert_pass",
    )(side, u_rows, do_rows, gate_loc, lin_loc, out_loc)


def weight_grad_kernel(groups, carried, *refs):
    ins = refs[:5 * groups]
    sums = refs[5 * groups:5 * groups + carried]
    outs = refs[5 * groups + carried:]
    acc = [ref[0] for ref in sums] if carried else [None] * 3
    for g in range(groups):
        u_ref, do_ref, h_ref, da0_ref, da1_ref = ins[5 * g:5 * g + 5]
        terms = (dot_tn(u_ref[0], da0_ref[0]), dot_tn(u_ref[0], da1_ref[0]), dot_tn(h_ref[0], do_ref[0]))
        acc = [t if a is None else a + t for a, t in zip(acc, terms)]
    for ref, val in zip(outs, acc):
        ref[0] = val


def weight_grads(parts, carry=()):
    local_exp, slot_cap, width = parts[0][0].shape
    ff = parts[0][2].shape[2]
    splits = 1
    ff_blk = ff // splits
    row_block = pl.BlockSpec((1, slot_cap, width), lambda e, f: (e, 0, 0))
    ff_block = pl.BlockSpec((1, slot_cap, ff_blk), lambda e, f: (e, 0, f))
    in_shape = jax.ShapeDtypeStruct((local_exp, width, ff), jnp.float32)
    out_shape = jax.ShapeDtypeStruct((local_exp, ff, width), jnp.float32)
    grad_specs = [pl.BlockSpec((1, width, ff_blk), lambda e, f: (e, 0, f)),
                  pl.BlockSpec((1, width, ff_blk), lambda e, f: (e, 0, f)),
                  pl.BlockSpec((1, ff_blk, width), lambda e, f: (e, f, 0))]
    first = 5 * len(parts)
    return pl.pallas_call(
        functools.partial(weight_grad_kernel, len(parts), len(carry)),
        grid=(local_exp, splits),
        in_specs=[row_block, row_block, ff_block, ff_block, ff_block] * len(parts) + (grad_specs if carry else []),
        out_specs=grad_specs,
        out_shape=[in_shape, in_shape, out_shape],
        input_output_aliases={first + i: i for i in range(len(carry))},
        compiler_params=pltpu.CompilerParams(vmem_limit_bytes=VMEM_LIMIT,
                                             dimension_semantics=("arbitrary", "arbitrary")),
        cost_estimate=pl.CostEstimate(flops=50_000_000_000, bytes_accessed=150_000_000, transcendentals=0),
        name="weight_grads",
    )(*[a for part in parts for a in part], *carry)


def rows_to_cols(rows):
    return jnp.transpose(rows, (1, 0))


def lane_pack(cols, lanes=LANES):
    count = cols[0].shape[0]
    lane = lax.broadcasted_iota(jnp.int32, (count, lanes), 1)
    packed = jnp.zeros((count, lanes), jnp.float32)
    for i, col in enumerate(cols):
        packed = jnp.where(lane == i, col, packed)
    return jnp.transpose(packed, (1, 0))[:8]


def fill_table(step, steps_each, sources, table):
    blk, slot_cap, half = sources[0].shape
    slices = half // LANES
    for g, src in enumerate(sources):
        @pl.when(step // steps_each == g)
        def _():
            rows = blk * slot_cap
            vals = src[...].reshape(rows, half).astype(jnp.float32)
            base = pl.multiple_of(step * (rows * slices), 8)
            for k in range(slices):
                table[pl.ds(base + k, rows, stride=slices), :] = vals[:, k * LANES:(k + 1) * LANES]


def pick_table(table, buf, row_ref, first, count, slices):
    unroll = 16

    def body(i, carry):
        for q in range(unroll):
            tok = i * unroll + q
            buf[pl.ds(pl.multiple_of(tok * slices, slices), slices), :] = \
                table[pl.ds(pl.multiple_of(row_ref[first + tok] * slices, slices), slices), :]
        return carry

    lax.fori_loop(0, count // unroll, body, 0)


def buf_slice(buf, k, count, slices):
    return buf[pl.ds(k, count, stride=slices), :]


def combine_o_kernel(table_steps, groups, row1_ref, row2_ref, side_ref, *refs):
    sources, (x_ref, dy_ref, feat_ref, y_ref, part_ref, table, buf1, buf2) = refs[:groups], refs[groups:]
    step = pl.program_id(0)
    count, half = x_ref.shape
    slices = half // LANES

    @pl.when(step == 0)
    def _():
        zero_at = table.shape[0] - 8
        table[pl.ds(zero_at, 8), :] = jnp.zeros((8, LANES), jnp.float32)

    @pl.when(step < table_steps)
    def _():
        fill_table(step, table_steps // groups, sources, table)

    @pl.when(step >= table_steps)
    def _():
        first = (step - table_steps) * count
        pick_table(table, buf1, row1_ref, first, count, slices)
        pick_table(table, buf2, row2_ref, first, count, slices)
        feat = rows_to_cols(feat_ref[...])
        n1, n2 = feat[:, 0:1], feat[:, 1:2]
        dn1 = dn2 = 0.0
        for k in range(slices):
            cols = slice(k * LANES, (k + 1) * LANES)
            o1 = buf_slice(buf1, k, count, slices)
            o2 = buf_slice(buf2, k, count, slices)
            dy = dy_ref[:, cols].astype(jnp.float32)
            y_ref[:, cols] = (x_ref[:, cols].astype(jnp.float32) + n1 * o1 + n2 * o2).astype(jnp.bfloat16)
            dn1 = dn1 + dy * o1
            dn2 = dn2 + dy * o2
        part_ref[...] = lane_pack([jnp.sum(dn1, axis=-1, keepdims=True), jnp.sum(dn2, axis=-1, keepdims=True)])


def combine_du_kernel(table_steps, groups, row1_ref, row2_ref, side_ref, *refs):
    sources = refs[:groups]
    (x_ref, feat_ref, dl_ref, wr_ref, scale_ref, du_ref, part_ref, dr_ref, ds_ref, table, buf1, buf2) = refs[groups:]
    step = pl.program_id(0)
    count, half = x_ref.shape
    slices = half // LANES

    @pl.when(step == 0)
    def _():
        zero_at = table.shape[0] - 8
        table[pl.ds(zero_at, 8), :] = jnp.zeros((8, LANES), jnp.float32)
        dr_ref[...] = jnp.zeros_like(dr_ref)
        ds_ref[...] = jnp.zeros_like(ds_ref)

    @pl.when(step < table_steps)
    def _():
        fill_table(step, table_steps // groups, sources, table)

    @pl.when(step >= table_steps)
    def _():
        first = (step - table_steps) * count
        pick_table(table, buf1, row1_ref, first, count, slices)
        pick_table(table, buf2, row2_ref, first, count, slices)
        inv_rms = rows_to_cols(feat_ref[...])[:, 2:3]
        d_logits = dl_ref[...]
        routed = lax.dot_general(d_logits, wr_ref[...], (((0,), (0,)), ((), ())), preferred_element_type=jnp.float32)
        dot = 0.0
        norm_in = []
        for k in range(slices):
            cols = slice(k * LANES, (k + 1) * LANES)
            du_exp = buf_slice(buf1, k, count, slices) + buf_slice(buf2, k, count, slices)
            xn = x_ref[:, cols].astype(jnp.float32) * inv_rms
            scaled = xn * scale_ref[:, cols]
            du_all = du_exp + routed[:, cols]
            du_ref[:, cols] = du_all
            dot = dot + du_all * scaled
            ds_ref[:, cols] += jnp.sum(du_all * xn, axis=0, keepdims=True)
            norm_in.append(scaled.astype(jnp.bfloat16).astype(jnp.float32))
        part_ref[...] = lane_pack([jnp.sum(dot, axis=-1, keepdims=True)])
        dr_ref[...] += jnp.dot(d_logits, jnp.concatenate(norm_in, axis=1), preferred_element_type=jnp.float32)


def finish_dx_kernel(side_ref, du_ref, x_ref, dy_ref, feat_ref, part_a_ref, part_b_ref, scale_ref, dx_ref):
    width = 2 * x_ref.shape[1]
    inv_rms = rows_to_cols(feat_ref[...])[:, 2:3]
    mean = rows_to_cols(part_a_ref[...] + part_b_ref[...])[:, 0:1] * (1.0 / width)
    xn = x_ref[...].astype(jnp.float32) * inv_rms
    grad = dy_ref[...].astype(jnp.float32) + inv_rms * (du_ref[...] * scale_ref[...] - xn * mean)
    dx_ref[...] = grad.astype(jnp.bfloat16)


TOK_BLOCK = 512


def half_specs(offset):
    at = lambda i: jnp.maximum(i - offset, 0)
    tok = lambda i, r1, r2, sd: (at(i), 0)
    half_tok = lambda i, r1, r2, sd: (at(i), sd[0])
    row = lambda i, r1, r2, sd: (0, at(i))
    return tok, half_tok, row


def combine_call(kernel, rows, side, sources, extra, extra_specs, outs, out_specs, tok_count):
    local_exp, slot_cap, half = sources[0].shape
    groups = len(sources)
    blk = 2
    each = local_exp // blk
    table_steps = groups * each
    slices = half // LANES
    src_specs = [pl.BlockSpec((blk, slot_cap, half), (lambda g: lambda i, r1, r2, sd: (jnp.clip(i - g * each, 0, each - 1), 0, 0))(g))
                 for g in range(groups)]
    return pl.pallas_call(
        functools.partial(kernel, table_steps, groups),
        grid_spec=pltpu.PrefetchScalarGridSpec(
            num_scalar_prefetch=3,
            grid=(table_steps + tok_count // TOK_BLOCK,),
            in_specs=src_specs + extra_specs(table_steps),
            out_specs=out_specs(table_steps),
            scratch_shapes=[
                pltpu.VMEM((groups * local_exp * slot_cap * slices + 8, LANES), jnp.float32),
                pltpu.VMEM((TOK_BLOCK * slices, LANES), jnp.float32),
                pltpu.VMEM((TOK_BLOCK * slices, LANES), jnp.float32),
            ],
        ),
        out_shape=outs,
        compiler_params=pltpu.CompilerParams(vmem_limit_bytes=VMEM_LIMIT, dimension_semantics=("arbitrary",)),
        cost_estimate=pl.CostEstimate(flops=50_000_000_000, bytes_accessed=40_000_000, transcendentals=0),
    )(rows[0], rows[1], side, *sources, *extra)


def combine_o(rows, side, sources, x_loc, dy_loc, feat):
    tok_count, width = x_loc.shape
    half = width // 2

    def ins(offset):
        _, half_tok, row = half_specs(offset)
        return [pl.BlockSpec((TOK_BLOCK, half), half_tok)] * 2 + [pl.BlockSpec((8, TOK_BLOCK), row)]

    def out_specs(offset):
        tok, _, row = half_specs(offset)
        return [pl.BlockSpec((TOK_BLOCK, half), tok), pl.BlockSpec((8, TOK_BLOCK), row)]

    outs = [jax.ShapeDtypeStruct((tok_count, half), jnp.bfloat16), jax.ShapeDtypeStruct((8, tok_count), jnp.float32)]
    return combine_call(combine_o_kernel, rows, side, sources, (x_loc, dy_loc, feat), ins, outs, out_specs, tok_count)


def combine_du(rows, side, sources, x_loc, feat, d_logits_t, router_half_t, scale_half):
    tok_count, width = x_loc.shape
    half = width // 2
    experts = d_logits_t.shape[0]
    whole = lambda i, r1, r2, sd: (0, 0)

    def ins(offset):
        _, half_tok, row = half_specs(offset)
        return [pl.BlockSpec((TOK_BLOCK, half), half_tok), pl.BlockSpec((8, TOK_BLOCK), row),
                pl.BlockSpec((experts, TOK_BLOCK), row), pl.BlockSpec((experts, half), whole),
                pl.BlockSpec((1, half), whole)]

    def out_specs(offset):
        tok, _, row = half_specs(offset)
        return [pl.BlockSpec((TOK_BLOCK, half), tok), pl.BlockSpec((8, TOK_BLOCK), row),
                pl.BlockSpec((experts, half), whole), pl.BlockSpec((1, half), whole)]

    outs = [jax.ShapeDtypeStruct((tok_count, half), jnp.float32), jax.ShapeDtypeStruct((8, tok_count), jnp.float32),
            jax.ShapeDtypeStruct((experts, half), jnp.float32), jax.ShapeDtypeStruct((1, half), jnp.float32)]
    return combine_call(combine_du_kernel, rows, side, sources,
                        (x_loc, feat, d_logits_t, router_half_t, scale_half), ins, outs, out_specs, tok_count)


def finish_dx(side, du_all, x_loc, dy_loc, feat, part_a, part_b, scale_half):
    tok_count, half = du_all.shape
    tok = lambda i, sd: (i, 0)
    half_tok = lambda i, sd: (i, sd[0])
    row = lambda i, sd: (0, i)
    return pl.pallas_call(
        finish_dx_kernel,
        grid_spec=pltpu.PrefetchScalarGridSpec(
            num_scalar_prefetch=1,
            grid=(tok_count // TOK_BLOCK,),
            in_specs=[pl.BlockSpec((TOK_BLOCK, half), tok), pl.BlockSpec((TOK_BLOCK, half), half_tok),
                      pl.BlockSpec((TOK_BLOCK, half), half_tok)] + [pl.BlockSpec((8, TOK_BLOCK), row)] * 3 +
                     [pl.BlockSpec((1, half), lambda i, sd: (0, 0))],
            out_specs=pl.BlockSpec((TOK_BLOCK, half), tok),
        ),
        out_shape=jax.ShapeDtypeStruct((tok_count, half), jnp.bfloat16),
        compiler_params=pltpu.CompilerParams(vmem_limit_bytes=VMEM_LIMIT, dimension_semantics=("arbitrary",)),
        cost_estimate=pl.CostEstimate(flops=10_000_000_000, bytes_accessed=20_000_000, transcendentals=0),
        name="finish_dx",
    )(side, du_all, x_loc, dy_loc, feat, part_a, part_b, scale_half)


def strict_lower(size):
    idx = jnp.arange(size, dtype=jnp.int32)
    return (idx[None, :] < idx[:, None]).astype(jnp.bfloat16)


def slot_positions(one_first, one_second):
    tok_count, experts = one_first.shape
    blk = 128
    hits = jnp.concatenate([one_first, one_second], axis=1)
    blocks = hits.astype(jnp.bfloat16).reshape(tok_count // blk, blk, 2 * experts)
    inner = jnp.einsum('ij,bje->bie', strict_lower(blk), blocks, preferred_element_type=jnp.float32)
    totals = jnp.sum(blocks.astype(jnp.float32), axis=1)
    outer = jnp.dot(strict_lower(tok_count // blk), totals.astype(jnp.bfloat16), preferred_element_type=jnp.float32)
    first_total = jnp.sum(totals[:, :experts], axis=0)
    shift = jnp.concatenate([jnp.zeros_like(first_total), first_total])
    rank = (inner + (outer + shift)[:, None, :]).reshape(tok_count, 2 * experts) * hits
    pos_first = jnp.sum(rank[:, :experts], axis=1).astype(jnp.int32)
    pos_second = jnp.sum(rank[:, experts:], axis=1).astype(jnp.int32)
    return pos_first, pos_second, first_total


def round_bf16(val):
    return lax.reduce_precision(val, 8, 7)


def solution(mesh):
    ep_size = mesh.shape['ep']
    tp_size = mesh.shape['tp']

    def swap_ep(val, bit):
        return lax.ppermute(val, 'ep', [(i, i ^ bit) for i in range(ep_size)])

    def swap_tp(val):
        return lax.ppermute(val, 'tp', [(i, i ^ 1) for i in range(tp_size)])

    def device_body(x_loc, dy_loc, idx_loc, norm_scale, w_router, gate_loc, lin_loc, out_loc):
        tok_count, width = x_loc.shape
        experts = w_router.shape[1]
        local_exp = gate_loc.shape[0]
        tokens = tok_count * ep_size
        slot_cap = (5 * tok_count + 2 * experts - 1) // (2 * experts)
        half = width // 2
        me = lax.axis_index('ep')
        side = lax.axis_index('tp')
        side_arr = side.astype(jnp.int32).reshape(1)

        quarter = tok_count // 4
        dy_half = lax.dynamic_slice_in_dim(dy_loc, side * (tok_count // 2), tok_count // 2, axis=0)
        dy2_p = swap_ep(dy_half[:quarter], 2)
        dy2_q = swap_ep(dy_half[quarter:], 2)
        x2 = swap_ep(x_loc, 2)
        dy2_r = swap_tp(dy2_p)
        dy2_s = swap_tp(dy2_q)
        x1 = swap_ep(x_loc, 1)
        dy1 = swap_ep(dy_loc, 1)
        x3 = swap_ep(x2, 1)
        dy2 = (dy2_p, dy2_q, dy2_r, dy2_s)
        dy3 = tuple(swap_ep(d, 1) for d in dy2)
        x_grp = (x_loc, x1, x2, x3)
        dy_grp = ((dy_loc,), (dy1,), dy2, dy3)

        x_wide = x_loc.astype(jnp.float32)
        inv_rms = lax.rsqrt(jnp.mean(x_wide * x_wide, axis=-1, keepdims=True) + NORM_EPS)
        u_tok = (x_wide * inv_rms * norm_scale).astype(jnp.bfloat16)
        u_wide = u_tok.astype(jnp.float32)
        logits = jnp.dot(u_wide, w_router, preferred_element_type=jnp.float32)
        log_norm = jax.nn.logsumexp(logits, axis=-1)
        router_prob = jnp.exp(logits - log_norm[:, None])
        expert_ids = jnp.arange(experts, dtype=jnp.int32)
        hit_first = idx_loc[:, 0:1] == expert_ids
        hit_second = idx_loc[:, 1:2] == expert_ids
        one_first = hit_first.astype(jnp.float32)
        one_second = hit_second.astype(jnp.float32)
        gate_first = jnp.sum(router_prob * one_first, axis=-1)
        gate_second = jnp.sum(router_prob * one_second, axis=-1)
        gate_total = gate_first + gate_second
        norm_first = gate_first / gate_total
        norm_second = gate_second / gate_total

        pos_first, pos_second, first_total = slot_positions(one_first, one_second)
        tok_ids = jnp.arange(tok_count, dtype=jnp.int32)
        tok_hi = (tok_ids // 64).astype(jnp.float32)
        tok_lo = (tok_ids % 64).astype(jnp.float32)
        slot_ids = jnp.arange(slot_cap, dtype=jnp.int32)
        table = 0.0
        for one, pos, norm in ((one_first, pos_first, norm_first), (one_second, pos_second, norm_second)):
            g_hi = round_bf16(norm)
            g_mid = round_bf16(norm - g_hi)
            g_lo = round_bf16(norm - g_hi - g_mid)
            feats = [jnp.ones_like(norm), tok_hi, tok_lo, g_hi, g_mid, g_lo]
            left = jnp.concatenate([one * f[:, None] for f in feats], axis=1).astype(jnp.bfloat16)
            right = (pos[:, None] == slot_ids).astype(jnp.bfloat16)
            table = table + lax.dot_general(left, right, (((0,), (0,)), ((), ())), preferred_element_type=jnp.float32)
        table = table.reshape(6, experts, slot_cap)
        slot_tok = jnp.where(table[0] > 0.5, table[1] * 64.0 + table[2], float(tok_count))
        slot_gate = table[3] + table[4] + table[5]
        slot_pack = jnp.stack([slot_tok, slot_gate]).reshape(2, ep_size, local_exp, slot_cap)
        stats = jnp.concatenate([first_total, jnp.sum(router_prob, axis=0), jnp.sum(log_norm * log_norm).reshape(1)])
        stats_row = jnp.pad(stats, (0, local_exp * slot_cap - stats.shape[0])).reshape(1, local_exp, slot_cap)
        grp_stats = []

        scale_row = norm_scale.reshape(1, width)
        near = ep_size // 2
        saved = {}
        back_o = [None] * ep_size
        back_du = [None] * ep_size
        sent = {}
        for bit in range(ep_size):
            pack = lax.dynamic_index_in_dim(slot_pack, me ^ bit, axis=1, keepdims=False)
            pack = jnp.concatenate([pack, stats_row])
            if bit:
                pack = swap_ep(pack, bit)
            if bit == near:
                grads = weight_grads([saved[b] for b in range(near)])
                after_near = grads[2][0, 0, :8]
            if bit >= near:
                pack, _ = lax.optimization_barrier((pack, after_near))
            grp_stats.append(pack[2].reshape(local_exp * slot_cap)[:stats.shape[0]])
            tok_grp = pack[0].astype(jnp.int32).reshape(local_exp * slot_cap)
            gate_grp = pack[1].reshape(local_exp, slot_cap, 1)
            u_rows, do_rows = gather_rows(tok_grp, side_arr, x_grp[bit], dy_grp[bit], scale_row, gate_grp)
            o_keep, o_send, du_keep, du_send, h, da0, da1 = run_experts(
                side_arr, u_rows, do_rows, gate_loc, lin_loc, out_loc)
            saved[bit] = (u_rows, do_rows, h, da0, da1)
            sent[bit] = (o_keep, o_send, du_keep, du_send)
        for bit in range(ep_size):
            o_keep, o_send, du_keep, du_send = sent[bit]
            o_got = swap_tp(o_send)
            du_got = swap_tp(du_send)
            o_sum = (o_keep.astype(jnp.float32) + o_got.astype(jnp.float32)).astype(jnp.bfloat16)
            du_sum = (du_keep.astype(jnp.float32) + du_got.astype(jnp.float32)).astype(jnp.bfloat16)
            if bit:
                o_sum = swap_ep(o_sum, bit)
                du_sum = swap_ep(du_sum, bit)
            back_o[bit] = o_sum
            back_du[bit] = du_sum
        d_gate, d_lin, d_out = weight_grads([saved[b] for b in range(near, ep_size)], grads)

        per_dev = local_exp * slot_cap

        def slot_row(exp_idx, pos):
            row = ((exp_idx // local_exp) ^ me) * per_dev + (exp_idx % local_exp) * slot_cap + pos
            return jnp.where(pos < slot_cap, row, ep_size * per_dev)

        rows = (slot_row(idx_loc[:, 0], pos_first), slot_row(idx_loc[:, 1], pos_second))
        half_of = lambda val, axis: lax.dynamic_slice_in_dim(val, side * half, half, axis=axis)
        scale_half = half_of(norm_scale, 0)[None, :]
        zero_row = jnp.zeros_like(norm_first)
        feat = jnp.stack([norm_first, norm_second, inv_rms[:, 0]] + [zero_row] * 5)
        y_half, part_o = combine_o(rows, side_arr, back_o, x_loc, dy_loc, feat)
        y_other = swap_tp(y_half)
        part_o = part_o + swap_tp(part_o)
        dn_first, dn_second = part_o[0], part_o[1]

        stats = (grp_stats[0] + grp_stats[1]) + (grp_stats[2] + grp_stats[3])
        first_count, prob_sum, norm_sq = stats[:experts], stats[experts:2 * experts], stats[2 * experts]
        frac_first = first_count / tokens
        z_loss = Z_COEF * norm_sq / tokens
        aux_loss = AUX_COEF * experts * jnp.sum(frac_first * prob_sum) / tokens
        gate_mix = norm_first * dn_first + norm_second * dn_second
        aux_coef = AUX_COEF * experts * frac_first
        d_logits = router_prob * (aux_coef - jnp.sum(aux_coef * router_prob, axis=-1, keepdims=True))
        d_logits = d_logits + (2.0 * Z_COEF) * log_norm[:, None] * router_prob
        d_logits = d_logits + one_first * (norm_first * (dn_first - gate_mix))[:, None]
        d_logits = d_logits + one_second * (norm_second * (dn_second - gate_mix))[:, None]

        du_all, part_du, d_router_half, d_scale_half = combine_du(
            rows, side_arr, back_du, x_loc, feat, d_logits.T, half_of(w_router, 0).T, scale_half)
        part_other = swap_tp(part_du)
        dx_half = finish_dx(side_arr, du_all, x_loc, dy_loc, feat, part_du, part_other, scale_half)
        dx_other = swap_tp(dx_half)
        sums = jnp.concatenate([d_router_half, d_scale_half])
        sums = sums + swap_ep(sums, 1)
        sums = sums + swap_ep(sums, 2)
        sums_other = swap_tp(sums)
        sums = jnp.where(side == 0, jnp.concatenate([sums, sums_other], axis=1), jnp.concatenate([sums_other, sums], axis=1))
        d_router = sums[:experts].T
        d_scale = sums[experts]

        def join(mine, other):
            return jnp.where(side == 0, jnp.concatenate([mine, other], axis=1), jnp.concatenate([other, mine], axis=1))

        y_loc = join(y_half, y_other)
        dx_loc = join(dx_half, dx_other)
        losses = jnp.stack([z_loss, aux_loss])
        return (y_loc, losses, dx_loc, d_scale, d_router, d_gate, d_lin, d_out)

    tok_spec = P('ep', None)
    in_spec = P('ep', None, 'tp')
    out_spec = P('ep', 'tp', None)
    return jax.shard_map(device_body, mesh=mesh, in_specs=(tok_spec, tok_spec, tok_spec, P(), P(), in_spec, in_spec, out_spec), out_specs=(tok_spec, P(), tok_spec, P(), P(), in_spec, in_spec, out_spec), check_vma=False)
```
